32 devices in a mesh: cp: 32 (over z, y, x, core).
Axes of the slice: x: 2, y: 2, z: 4, core: 2. Of those that a mesh axis runs over, the one named last changes fastest.
Arguments:
- raw_inputs: bfloat16 [3584, 57344], P(None, 'cp'), may hold values from -6 to 6
- state_maps: bfloat16 [128, 57344], P(None, 'cp'), may hold values from -6 to 6
- step_size: float32 [56, 57344], P(None, 'cp'), may hold values from 0 to 1, as said below
- log_decay: float32 [56, 57344], P(None, 'cp'), may hold values from -2 to 0, as said below
- conv_weight: float32 [4, 3584], replicated, may hold values from -3 to 3
- conv_bias: float32 [3584], replicated, may hold values from -3 to 3
- skip_gain: float32 [56], replicated, may hold values from 0.5 to 1.5
Outputs:
- layer_output: bfloat16 [3584, 57344], P(None, 'cp')
The draws below stay inside these ranges and needn't reach their ends.
Inputs may be any that keep to these rules, and one draw needn't show every extreme that they name: step_size is positive. log_decay is never positive.
All inputs are finite; a program needn't handle non-finite values.
Results may differ from the reference program's by a relative error of at most 0.0058.
Values may be sent and summed in bfloat16 or wider, within the bound.
A program may use at most 192 MiB of HBM per device.

```python
import jax
import jax.numpy as jnp
from jax import lax

HEADS = 56
HEAD_DIM = 64
STATE = 64
BLOCK = 256
CONVOLUTION_TAPS = 4
TOK_DEV = 1792
TOKENS = 57344


def decay_and_step(key):
    folded = jax.random.fold_in(key, 41)
    subkeys = jax.random.split(folded, 7)
    ranking = jax.random.permutation(subkeys[0], HEADS)
    slow_heads = ranking < HEADS // 2
    chain_total = jnp.exp(jax.random.uniform(subkeys[1], (HEADS,), jnp.float32, jnp.log(0.3), jnp.log(0.9)))
    slow_rate = chain_total / (1.0 * TOKENS)
    fast_rate = jnp.exp(jax.random.uniform(subkeys[2], (HEADS,), jnp.float32, jnp.log(1.0 / 50.0), jnp.log(1.0 / 30.0)))
    decay_rate = jnp.where(slow_heads, slow_rate, fast_rate)
    head_step = jnp.where(slow_heads, 0.2 / jnp.sqrt(1.0 * TOKENS), 0.2 * jnp.sqrt(2.0 * fast_rate))
    blocks = TOKENS // TOK_DEV
    device_factor = jnp.exp(jax.random.uniform(subkeys[3], (HEADS, blocks), jnp.float32, -0.5, 0.5))
    device_factor = jnp.repeat(device_factor, TOK_DEV, axis=1)
    token_factor = jax.random.uniform(subkeys[4], (HEADS, TOKENS), jnp.float32, 0.5, 1.5)
    logarithmic_decay = -(decay_rate[:, None] * device_factor * token_factor)
    device_positions = jax.random.randint(subkeys[5], (3, HEADS), 0, TOKENS)
    training_losses = jax.random.uniform(subkeys[6], (3, HEADS), jnp.float32, 0.22, 0.43)
    token_position = lax.broadcasted_iota(jnp.int32, (HEADS, TOKENS), 1)
    for segment_index in range(3):
        logarithmic_decay = logarithmic_decay - jnp.where(token_position == device_positions[segment_index][:, None], training_losses[segment_index][:, None], 0.0)
    step_sizes = head_step[:, None] * token_factor
    return (logarithmic_decay, step_sizes)


def draw_step_size(key, part):
    return decay_and_step(key)[1].astype(jnp.float32)


def draw_log_decay(key, part):
    return decay_and_step(key)[0].astype(jnp.float32)


def shard_levels(stream_key, dims, shards, least, top_value):
    loudness, own = 1.0, jax.random.fold_in(stream_key, 6)
    for axis_at, parts in shards:
        heights = jnp.exp(jax.random.uniform(jax.random.fold_in(own, axis_at), (parts,), jnp.float32, least / len(shards), top_value / len(shards)))
        loudness = loudness * jnp.repeat(heights, dims[axis_at] // parts).reshape([-1 if axis == axis_at else 1 for axis in range(len(dims))])
    return loudness


def noise(stream_key, extent, deviation, reach, cuts=(), held_as=jnp.bfloat16):
    factor_of = shard_levels(stream_key, extent, cuts, -0.22, 0.18) if cuts else 1.0
    array = jax.random.normal(stream_key, extent, jnp.float32) * deviation * factor_of
    return jnp.minimum(jnp.maximum(array, -reach), reach).astype(held_as)


def setup_inputs(seed: int = 0) -> dict:
    key_of = jax.random.split(jax.random.key(seed), 8)
    return {
        "raw_inputs": noise(key_of[0], (HEADS * HEAD_DIM, TOKENS), 1.0, 6.0, ((1, 32),)),
        "state_maps": noise(key_of[1], (2 * STATE, TOKENS), 1.0, 6.0, ((1, 32),)),
        "step_size": draw_step_size(jax.random.fold_in(key_of[7], 71), 0),
        "log_decay": draw_log_decay(jax.random.fold_in(key_of[7], 71), 0),
        "conv_weight": noise(key_of[4], (CONVOLUTION_TAPS, HEADS * HEAD_DIM), CONVOLUTION_TAPS ** -0.5, 3.0, (), jnp.float32),
        "conv_bias": noise(key_of[5], (HEADS * HEAD_DIM,), 0.5, 3.0, (), jnp.float32),
        "skip_gain": jnp.clip(jax.random.uniform(key_of[6], (HEADS,), jnp.float32, 0.5, 1.5), 0.5, 1.5),
    }


def reference(raw_inputs, state_maps, step_size, log_decay, conv_weight, conv_bias, skip_gain):
    conv_taps = conv_weight.shape[0]
    block_count = TOKENS // BLOCK
    channels = HEADS * HEAD_DIM
    raw_blocks = raw_inputs.T.reshape(block_count, BLOCK, channels)
    map_blocks = state_maps.T.reshape(block_count, BLOCK, 2 * STATE)
    step_blocks = jnp.transpose(step_size.reshape(HEADS, block_count, BLOCK), (1, 0, 2))
    decay_blocks = jnp.transpose(log_decay.reshape(HEADS, block_count, BLOCK), (1, 0, 2))
    causal = jnp.arange(BLOCK)[:, None] >= jnp.arange(BLOCK)[None, :]

    def advance(carry_in, pieces):
        state_now, prior_rows = carry_in
        block_raw, block_transforms, block_steps, block_decay = pieces
        extended = jnp.concatenate([prior_rows, block_raw], axis=0).astype(jnp.float32)
        convolved = jnp.zeros((BLOCK, channels), jnp.float32) + conv_bias[None, :]
        for offset in range(conv_taps):
            convolved = convolved + conv_weight[offset][None, :] * extended[offset:offset + BLOCK]
        values = jax.nn.silu(convolved).astype(jnp.bfloat16)
        inputs = values.reshape(BLOCK, HEADS, HEAD_DIM).astype(jnp.float32)
        key_rows = block_transforms[:, :STATE]
        query_rows = block_transforms[:, STATE:]
        sums = jnp.cumsum(block_decay, axis=1)
        affinity = jnp.dot(query_rows, key_rows.T, preferred_element_type=jnp.float32)
        decay_gaps = jnp.where(causal[None], sums[:, :, None] - sums[:, None, :], 0.0)
        weights = jnp.where(causal[None], affinity[None] * jnp.exp(decay_gaps) * block_steps[:, None, :], 0.0).astype(jnp.bfloat16)
        local_out = jnp.einsum("hij,jhp->ihp", weights.astype(jnp.float32), inputs)
        entering_b = state_now.astype(jnp.bfloat16).astype(jnp.float32)
        carried = jnp.einsum("in,hnp->ihp", query_rows.astype(jnp.float32), entering_b) * jnp.exp(sums).T[:, :, None]
        result_rows = local_out + carried + skip_gain[None, :, None] * inputs
        block_end = sums[:, BLOCK - 1:]
        scaled = (key_rows.astype(jnp.float32)[None] * (jnp.exp(block_end - sums) * block_steps)[:, :, None]).astype(jnp.bfloat16)
        block_state = jnp.einsum("hjn,jhp->hnp", scaled.astype(jnp.float32), inputs)
        next_state = jnp.exp(block_end)[:, :, None] * state_now + block_state
        next_rows = block_raw[BLOCK - (conv_taps - 1):]
        return (next_state, next_rows), result_rows.reshape(BLOCK, channels).astype(jnp.bfloat16)

    start_state = jnp.zeros((HEADS, STATE, HEAD_DIM), jnp.float32)
    start_rows = jnp.zeros((conv_taps - 1, channels), jnp.bfloat16)
    final_carry, outputs = lax.scan(advance, (start_state, start_rows), (raw_blocks, map_blocks, step_blocks, decay_blocks))
    return outputs.reshape(TOKENS, channels).T
```

```python
import functools

import jax
import jax.numpy as jnp
from jax import lax
from jax.experimental import pallas as pl
from jax.experimental.pallas import tpu as pltpu
from jax.sharding import PartitionSpec as P

HALF = 64
TILE = 128
PAIR = 256
GROUP = 8


def prepare_kernel(state_dim, decay_ref, step_ref, maps_ref, e_ref, b_ref, a0_ref, a1_ref, f_ref, d_ref,
                   total_ref, key_ref, mix_ref):
    tiles = decay_ref.shape[1] // TILE
    heads = decay_ref.shape[0]
    row = lax.broadcasted_iota(jnp.int32, (TILE, TILE), 0)
    col = lax.broadcasted_iota(jnp.int32, (TILE, TILE), 1)
    upper = (row <= col).astype(jnp.float32)
    same = (row <= col) & ((row < HALF) == (col < HALF))
    cross = (row < HALF) & (col >= HALF)
    lane = lax.broadcasted_iota(jnp.int32, (heads, TILE), 1)
    low_cols = lax.broadcasted_iota(jnp.int32, (state_dim, TILE), 1) < HALF
    total = jnp.zeros((heads, TILE), jnp.float32)
    for t in range(tiles):
        span = slice(t * TILE, (t + 1) * TILE)
        sums = jnp.dot(decay_ref[:, span], upper, precision=lax.Precision.HIGHEST,
                       preferred_element_type=jnp.float32)
        step = step_ref[:, span]
        first = jnp.broadcast_to(sums[:, HALF // 2 - 1:HALF // 2], (heads, TILE))
        second = jnp.broadcast_to(sums[:, HALF + HALF // 2 - 1:HALF + HALF // 2], (heads, TILE))
        end = jnp.broadcast_to(sums[:, TILE - 1:], (heads, TILE))
        middle = jnp.where(lane < HALF, first, second)
        e_ref[:, span] = jnp.exp(end - sums) * step
        b_ref[:, span] = jnp.exp(middle - sums) * step
        a0_ref[:, span] = jnp.exp(sums - middle)
        a1_ref[:, span] = jnp.where(lane < HALF, 0.0, jnp.exp(jnp.where(lane < HALF, 0.0, sums - first)))
        f_ref[:, span] = jnp.exp(first)
        d_ref[:, span] = jnp.exp(end)
        total = total + end
        keys = maps_ref[:state_dim, span]
        queries = maps_ref[state_dim:, span]
        keys_t = keys.astype(jnp.float32).T.astype(jnp.bfloat16)
        affinity = jnp.dot(keys_t, queries, preferred_element_type=jnp.float32)
        zero_keys = jnp.zeros_like(keys_t)
        side = [keys_t, zero_keys] if t % 2 == 0 else [zero_keys, keys_t]
        key_ref[t // 2, (t % 2) * TILE:(t % 2 + 1) * TILE, :] = jnp.concatenate(side, axis=1)
        mix_ref[t, :TILE, :TILE] = jnp.where(same, affinity, 0.0).astype(jnp.bfloat16)
        mix_ref[t, :TILE, TILE:] = jnp.where(cross, affinity, 0.0).astype(jnp.bfloat16)
        wide = queries.astype(jnp.float32)
        mix_ref[t, TILE:, :TILE] = jnp.where(low_cols, wide, 0.0).astype(jnp.bfloat16)
        mix_ref[t, TILE:, TILE:] = jnp.where(low_cols, 0.0, wide).astype(jnp.bfloat16)
    total_ref[...] = total


def rows_of(vector, head_dim):
    count, width = vector.shape
    return jnp.broadcast_to(vector[:, None, :], (count, head_dim, width)).reshape(count * head_dim, width)


def state_kernel(head_dim, state_dim, raw_ref, side_ref, e_ref, d_ref, total_ref, key_ref, x_ref, part_ref,
                 message_ref, column_ref, scaled_ref, spread_ref):
    rows, tokens = raw_ref.shape
    tiles = tokens // TILE
    side = side_ref[...]
    padded = jnp.concatenate([jnp.zeros((TILE - side.shape[0], rows), jnp.float32), side], axis=0)
    column_ref[...] = padded.T
    spread_ref[...] = rows_of(e_ref[...], 8)
    step_rows = head_dim // 2
    base = TILE - side.shape[0]

    def convolve(group, carry):
        start = pl.multiple_of(group * step_rows, step_rows)
        head = group // 2
        lane = lax.broadcasted_iota(jnp.int32, (step_rows, TILE), 1)
        columns = column_ref[pl.ds(start, step_rows), :]
        w0, w1, w2, w3, bias = [
            jnp.broadcast_to(columns[:, base + k:base + k + 1], (step_rows, TILE)) for k in range(5)
        ]
        before1 = pltpu.roll(columns, 1, 1)
        before2 = pltpu.roll(w1 * columns + w0 * before1, 2, 1)
        for t in range(tiles):
            span = slice(t * TILE, (t + 1) * TILE)
            now = raw_ref[pl.ds(start, step_rows), span].astype(jnp.float32)
            turned = pltpu.roll(now, 1, 1)
            late1 = jnp.where(lane < 1, before1, turned)
            before1 = turned
            turned = pltpu.roll(w1 * now + w0 * late1, 2, 1)
            late2 = jnp.where(lane < 2, before2, turned)
            before2 = turned
            half = (bias + w3 * now) + (w2 * late1 + late2)
            value = half + half * jnp.tanh(half)
            weight = jnp.concatenate([spread_ref[pl.ds(pl.multiple_of(head * 8, 8), 8), span]] * (step_rows // 8), axis=0)
            x_ref[pl.ds(start, step_rows), span] = value.astype(jnp.bfloat16)
            scaled_ref[pl.ds(start, step_rows), span] = (value * weight).astype(jnp.bfloat16)
        return carry

    lax.fori_loop(0, rows // step_rows, convolve, 0)
    state = jnp.zeros((rows, state_dim), jnp.float32)
    for k in range(tokens // PAIR):
        part = jnp.dot(scaled_ref[:, k * PAIR:(k + 1) * PAIR], key_ref[k], preferred_element_type=jnp.float32)
        part_ref[:, k * TILE:(k + 1) * TILE] = part.astype(jnp.bfloat16)
        for i in range(2):
            decay = rows_of(d_ref[:, (2 * k + i) * TILE:(2 * k + i) * TILE + state_dim], head_dim)
            state = decay * state + part[:, i * state_dim:(i + 1) * state_dim]
    total = rows_of(total_ref[:, :state_dim], head_dim)
    high = total.astype(jnp.bfloat16)
    rest = total - high.astype(jnp.float32)
    middle = rest.astype(jnp.bfloat16)
    low = rest - middle.astype(jnp.float32)
    lane = lax.broadcasted_iota(jnp.int32, (rows, state_dim), 1)
    logs = jnp.where(lane == 0, high.astype(jnp.float32), jnp.where(lane == 1, middle.astype(jnp.float32), low))
    message_ref[...] = jnp.concatenate([state, logs], axis=1).astype(jnp.bfloat16)


def combine_kernel(state_dim, got_ref, out_ref):
    peers, rows, width = got_ref.shape
    running = jnp.zeros((rows, width), jnp.float32)
    for d in range(peers):
        out_ref[d] = running.astype(jnp.bfloat16)
        got = got_ref[d].astype(jnp.float32)
        log = (got[:, state_dim:state_dim + 1] + got[:, state_dim + 1:state_dim + 2]) + got[:, state_dim + 2:state_dim + 3]
        running = jnp.exp(log) * running + got


def output_kernel(head_dim, state_dim, x_ref, part_ref, enter_ref, b_ref, a0_ref, a1_ref, f_ref, d_ref, gain_ref,
                  mix_ref, out_ref, state_ref):
    tokens = x_ref.shape[1]
    state_ref[...] = enter_ref[:, :state_dim].astype(jnp.float32)
    gain = rows_of(gain_ref[...], head_dim)

    def pair(k, carry):
        parts = part_ref[:, pl.ds(pl.multiple_of(k * TILE, TILE), TILE)].astype(jnp.float32)
        for i in range(2):
            span = pl.ds(pl.multiple_of(k * PAIR + i * TILE, TILE), TILE)
            x = x_ref[:, span].astype(jnp.float32)
            scaled = (x * rows_of(b_ref[:, span], head_dim)).astype(jnp.bfloat16)
            state = state_ref[...]
            entering = (state * rows_of(f_ref[:, span], head_dim)[:, :state_dim]).astype(jnp.bfloat16)
            left = jnp.concatenate([scaled, entering], axis=1)
            mixed = jnp.dot(left, mix_ref[2 * k + i], preferred_element_type=jnp.float32)
            out = mixed[:, :TILE] * rows_of(a0_ref[:, span], head_dim)
            out = out + mixed[:, TILE:] * rows_of(a1_ref[:, span], head_dim)
            out_ref[:, span] = (out + gain * x).astype(jnp.bfloat16)
            state_ref[...] = state * rows_of(d_ref[:, span], head_dim)[:, :state_dim] + parts[
                :, i * state_dim:(i + 1) * state_dim]
        return carry

    lax.fori_loop(0, tokens // PAIR, pair, 0)


def local(raw_inputs, state_maps, step_size, log_decay, conv_weight, conv_bias, skip_gain):
    taps = conv_weight.shape[0]
    channels, tokens = raw_inputs.shape
    heads = skip_gain.shape[0]
    head_dim = channels // heads
    state_dim = state_maps.shape[0] // 2
    peers = lax.axis_size("cp")
    tiles = tokens // TILE
    group_rows = GROUP * head_dim
    f32, bf16 = jnp.float32, jnp.bfloat16

    tail = raw_inputs[:, tokens - (taps - 1):].T
    halo = lax.ppermute(tail, "cp", [(s, s + 1) for s in range(peers - 1)])
    vector = jax.ShapeDtypeStruct((heads, tokens), f32)
    e, b, a0, a1, f, d, total, keys, mix = pl.pallas_call(
        functools.partial(prepare_kernel, state_dim),
        out_shape=[vector] * 6 + [
            jax.ShapeDtypeStruct((heads, TILE), f32),
            jax.ShapeDtypeStruct((tiles // 2, PAIR, 2 * state_dim), bf16),
            jax.ShapeDtypeStruct((tiles, TILE + state_dim, 2 * TILE), bf16),
        ],
        cost_estimate=pl.CostEstimate(flops=100000000, bytes_accessed=6000000, transcendentals=0),
    )(log_decay, step_size, state_maps)
    side = jnp.concatenate([0.5 * conv_weight, 0.5 * conv_bias[None], halo.astype(f32)], axis=0)

    grid = heads // GROUP
    wide = lambda cols: pl.BlockSpec((group_rows, cols), lambda g: (g, 0))
    vec = pl.BlockSpec((GROUP, tokens), lambda g: (g, 0))
    vec1 = pl.BlockSpec((GROUP, TILE), lambda g: (g, 0))
    full = lambda array: pl.BlockSpec(array.shape, lambda g: (0,) * array.ndim)
    x, part, message = pl.pallas_call(
        functools.partial(state_kernel, head_dim, state_dim),
        grid=(grid,),
        in_specs=[wide(tokens), pl.BlockSpec((side.shape[0], group_rows), lambda g: (0, g)), vec, vec, vec1, full(keys)],
        out_specs=[wide(tokens), wide(tiles * state_dim), wide(2 * state_dim)],
        out_shape=[
            jax.ShapeDtypeStruct((channels, tokens), bf16),
            jax.ShapeDtypeStruct((channels, tiles * state_dim), bf16),
            jax.ShapeDtypeStruct((channels, 2 * state_dim), bf16),
        ],
        scratch_shapes=[pltpu.VMEM((group_rows, TILE), f32), pltpu.VMEM((group_rows, tokens), bf16),
                        pltpu.VMEM((GROUP * 8, tokens), f32)],
        compiler_params=pltpu.CompilerParams(dimension_semantics=("arbitrary",)),
    )(raw_inputs, side, e, d, total, keys)

    send = message.reshape(peers, channels // peers, 2 * state_dim)
    got = lax.all_to_all(send, "cp", split_axis=0, concat_axis=0, tiled=True)
    before = pl.pallas_call(
        functools.partial(combine_kernel, state_dim),
        out_shape=jax.ShapeDtypeStruct(got.shape, bf16),
    )(got)
    returned = lax.all_to_all(before, "cp", split_axis=0, concat_axis=0, tiled=True)
    enter = returned.reshape(channels, 2 * state_dim)
    gain = jnp.broadcast_to(skip_gain[:, None], (heads, TILE))
    return pl.pallas_call(
        functools.partial(output_kernel, head_dim, state_dim),
        grid=(grid,),
        in_specs=[wide(tokens), wide(tiles * state_dim), wide(2 * state_dim), vec, vec, vec, vec, vec, vec1, full(mix)],
        out_specs=wide(tokens),
        out_shape=jax.ShapeDtypeStruct((channels, tokens), bf16),
        scratch_shapes=[pltpu.VMEM((group_rows, state_dim), f32)],
        compiler_params=pltpu.CompilerParams(dimension_semantics=("arbitrary",)),
    )(x, part, enter, b, a0, a1, f, d, gain, mix)


def solution(mesh):
    placed = (P(None, "cp"), P(None, "cp"), P(None, "cp"), P(None, "cp"), P(), P(), P())
    return jax.shard_map(
        local, mesh=mesh, in_specs=placed, out_specs=P(None, "cp"), check_vma=False
    )
```

```python
import functools

import jax
import jax.numpy as jnp
from jax import lax
from jax.experimental import pallas as pl
from jax.experimental.pallas import tpu as pltpu
from jax.sharding import PartitionSpec as P

HALF = 64
TILE = 128
PAIR = 256
GROUP = 8


def prepare_kernel(state_dim, decay_ref, step_ref, maps_ref, e_ref, b_ref, a0_ref, a1_ref, f_ref, d_ref,
                   total_ref, key_ref, mix_ref):
    tiles = decay_ref.shape[1] // TILE
    heads = decay_ref.shape[0]
    row = lax.broadcasted_iota(jnp.int32, (TILE, TILE), 0)
    col = lax.broadcasted_iota(jnp.int32, (TILE, TILE), 1)
    upper = (row <= col).astype(jnp.float32)
    same = (row <= col) & ((row < HALF) == (col < HALF))
    cross = (row < HALF) & (col >= HALF)
    lane = lax.broadcasted_iota(jnp.int32, (heads, TILE), 1)
    low_cols = lax.broadcasted_iota(jnp.int32, (state_dim, TILE), 1) < HALF
    total = jnp.zeros((heads, TILE), jnp.float32)
    for t in range(tiles):
        span = slice(t * TILE, (t + 1) * TILE)
        sums = jnp.dot(decay_ref[:, span], upper, precision=lax.Precision.HIGHEST,
                       preferred_element_type=jnp.float32)
        step = step_ref[:, span]
        first = jnp.broadcast_to(sums[:, HALF // 2 - 1:HALF // 2], (heads, TILE))
        second = jnp.broadcast_to(sums[:, HALF + HALF // 2 - 1:HALF + HALF // 2], (heads, TILE))
        end = jnp.broadcast_to(sums[:, TILE - 1:], (heads, TILE))
        middle = jnp.where(lane < HALF, first, second)
        e_ref[:, span] = jnp.exp(end - sums) * step
        b_ref[:, span] = jnp.exp(middle - sums) * step
        a0_ref[:, span] = jnp.exp(sums - middle)
        a1_ref[:, span] = jnp.where(lane < HALF, 0.0, jnp.exp(jnp.where(lane < HALF, 0.0, sums - first)))
        f_ref[:, span] = jnp.exp(first)
        d_ref[:, span] = jnp.exp(end)
        total = total + end
        keys = maps_ref[:state_dim, span]
        queries = maps_ref[state_dim:, span]
        keys_t = keys.astype(jnp.float32).T.astype(jnp.bfloat16)
        affinity = jnp.dot(keys_t, queries, preferred_element_type=jnp.float32)
        zero_keys = jnp.zeros_like(keys_t)
        side = [keys_t, zero_keys] if t % 2 == 0 else [zero_keys, keys_t]
        key_ref[t // 2, (t % 2) * TILE:(t % 2 + 1) * TILE, :] = jnp.concatenate(side, axis=1)
        mix_ref[t, :TILE, :TILE] = jnp.where(same, affinity, 0.0).astype(jnp.bfloat16)
        mix_ref[t, :TILE, TILE:] = jnp.where(cross, affinity, 0.0).astype(jnp.bfloat16)
        wide = queries.astype(jnp.float32)
        mix_ref[t, TILE:, :TILE] = jnp.where(low_cols, wide, 0.0).astype(jnp.bfloat16)
        mix_ref[t, TILE:, TILE:] = jnp.where(low_cols, 0.0, wide).astype(jnp.bfloat16)
    total_ref[...] = total


def rows_of(vector, head_dim):
    count, width = vector.shape
    return jnp.broadcast_to(vector[:, None, :], (count, head_dim, width)).reshape(count * head_dim, width)


def state_kernel(head_dim, state_dim, raw_ref, side_ref, e_ref, d_ref, key_ref, x_ref, part_ref, message_ref,
                 column_ref, scaled_ref, spread_ref):
    rows, tokens = raw_ref.shape
    tiles = tokens // TILE
    side = side_ref[...]
    padded = jnp.concatenate([jnp.zeros((TILE - side.shape[0], rows), jnp.float32), side], axis=0)
    column_ref[...] = padded.T
    spread_ref[...] = rows_of(e_ref[...], 8)
    step_rows = head_dim // 2
    base = TILE - side.shape[0]

    def convolve(group, carry):
        start = pl.multiple_of(group * step_rows, step_rows)
        head = group // 2
        lane = lax.broadcasted_iota(jnp.int32, (step_rows, TILE), 1)
        columns = column_ref[pl.ds(start, step_rows), :]
        w0, w1, w2, w3, bias = [
            jnp.broadcast_to(columns[:, base + k:base + k + 1], (step_rows, TILE)) for k in range(5)
        ]
        before1 = pltpu.roll(columns, 1, 1)
        before2 = pltpu.roll(w1 * columns + w0 * before1, 2, 1)
        for t in range(tiles):
            span = slice(t * TILE, (t + 1) * TILE)
            now = raw_ref[pl.ds(start, step_rows), span].astype(jnp.float32)
            turned = pltpu.roll(now, 1, 1)
            late1 = jnp.where(lane < 1, before1, turned)
            before1 = turned
            turned = pltpu.roll(w1 * now + w0 * late1, 2, 1)
            late2 = jnp.where(lane < 2, before2, turned)
            before2 = turned
            half = (bias + w3 * now) + (w2 * late1 + late2)
            value = half + half * jnp.tanh(half)
            weight = jnp.concatenate([spread_ref[pl.ds(pl.multiple_of(head * 8, 8), 8), span]] * (step_rows // 8), axis=0)
            x_ref[pl.ds(start, step_rows), span] = value.astype(jnp.bfloat16)
            scaled_ref[pl.ds(start, step_rows), span] = (value * weight).astype(jnp.bfloat16)
        return carry

    lax.fori_loop(0, rows // step_rows, convolve, 0)
    state = jnp.zeros((rows, state_dim), jnp.float32)
    for k in range(tokens // PAIR):
        part = jnp.dot(scaled_ref[:, k * PAIR:(k + 1) * PAIR], key_ref[k], preferred_element_type=jnp.float32)
        part_ref[:, k * TILE:(k + 1) * TILE] = part.astype(jnp.bfloat16)
        for i in range(2):
            decay = rows_of(d_ref[:, (2 * k + i) * TILE:(2 * k + i) * TILE + state_dim], head_dim)
            state = decay * state + part[:, i * state_dim:(i + 1) * state_dim]
    message_ref[...] = packed(state, head_dim).astype(jnp.bfloat16)


def packed(state, head_dim):
    rows, width = state.shape
    pieces = state.reshape(rows // head_dim, 2, head_dim // 2, width)
    return jnp.concatenate([pieces[:, 0], pieces[:, 1]], axis=2).reshape(rows // 2, 2 * width)


def unpacked(pairs, head_dim):
    rows, width = pairs.shape
    pieces = pairs.reshape(2 * rows // head_dim, head_dim // 2, width)
    return jnp.concatenate([pieces[:, :, :width // 2], pieces[:, :, width // 2:]], axis=1).reshape(
        2 * rows, width // 2)


def exchange_kernel(peers, own, message_ref, out_ref, got_ref, reply_ref, back_ref, log_ref,
                    send1, recv1, send2, recv2):
    me = lax.axis_index("cp")
    barrier = pltpu.get_barrier_semaphore()

    def greet(k, carry):
        pl.semaphore_signal(barrier, inc=1, device_id=(lax.rem(me + k, peers),),
                            device_id_type=pl.DeviceIdType.MESH)
        return carry

    lax.fori_loop(1, peers, greet, 0)
    pl.semaphore_wait(barrier, peers - 1)

    def outward(k):
        peer = lax.rem(me + k, peers)
        return pltpu.make_async_remote_copy(
            src_ref=message_ref.at[peer], dst_ref=got_ref.at[me], send_sem=send1.at[peer], recv_sem=recv1.at[me],
            device_id=(peer,), device_id_type=pl.DeviceIdType.MESH)

    def inward(k):
        peer = lax.rem(me + k, peers)
        return pltpu.make_async_remote_copy(
            src_ref=message_ref.at[peer], dst_ref=got_ref.at[peer], send_sem=send1.at[peer], recv_sem=recv1.at[peer],
            device_id=(peer,), device_id_type=pl.DeviceIdType.MESH)

    def reply(k):
        peer = lax.rem(me + k, peers)
        return pltpu.make_async_remote_copy(
            src_ref=reply_ref.at[peer], dst_ref=back_ref.at[me], send_sem=send2.at[peer], recv_sem=recv2.at[me],
            device_id=(peer,), device_id_type=pl.DeviceIdType.MESH)

    def answer(k):
        peer = lax.rem(me + k, peers)
        return pltpu.make_async_remote_copy(
            src_ref=reply_ref.at[peer], dst_ref=back_ref.at[peer], send_sem=send2.at[peer], recv_sem=recv2.at[peer],
            device_id=(peer,), device_id_type=pl.DeviceIdType.MESH)

    def each(action):
        def step(k, carry):
            action(k)
            return carry
        lax.fori_loop(1, peers, step, 0)

    each(lambda k: outward(k).start())
    got_ref[me] = message_ref[me]
    each(lambda k: inward(k).wait_recv())
    log_ref[...] = jnp.zeros_like(log_ref)
    for d in range(peers):
        logs = got_ref[d, own:own + 3].astype(jnp.float32)
        log_ref[d:d + 1] = (logs[0:1] + logs[1:2]) + logs[2:3]
    decays = jnp.exp(log_ref[...]).T
    running = jnp.zeros((own, got_ref.shape[2]), jnp.float32)
    for d in range(peers):
        reply_ref[d] = running.astype(jnp.bfloat16)
        running = decays[:own, d:d + 1] * running + got_ref[d, :own].astype(jnp.float32)
    each(lambda k: reply(k).start())
    back_ref[me] = reply_ref[me]
    each(lambda k: answer(k).wait_recv())
    out_ref[...] = back_ref[...]
    each(lambda k: outward(k).wait_send())
    each(lambda k: reply(k).wait_send())


def output_kernel(head_dim, state_dim, x_ref, part_ref, enter_ref, b_ref, a0_ref, a1_ref, f_ref, d_ref, gain_ref,
                  mix_ref, out_ref, state_ref):
    tokens = x_ref.shape[1]
    state_ref[...] = unpacked(enter_ref[...].astype(jnp.float32), head_dim)
    gain = rows_of(gain_ref[...], head_dim)

    def pair(k, carry):
        parts = part_ref[:, pl.ds(pl.multiple_of(k * TILE, TILE), TILE)].astype(jnp.float32)
        for i in range(2):
            span = pl.ds(pl.multiple_of(k * PAIR + i * TILE, TILE), TILE)
            x = x_ref[:, span].astype(jnp.float32)
            scaled = (x * rows_of(b_ref[:, span], head_dim)).astype(jnp.bfloat16)
            state = state_ref[...]
            entering = (state * rows_of(f_ref[:, span], head_dim)[:, :state_dim]).astype(jnp.bfloat16)
            left = jnp.concatenate([scaled, entering], axis=1)
            mixed = jnp.dot(left, mix_ref[2 * k + i], preferred_element_type=jnp.float32)
            out = mixed[:, :TILE] * rows_of(a0_ref[:, span], head_dim)
            out = out + mixed[:, TILE:] * rows_of(a1_ref[:, span], head_dim)
            out_ref[:, span] = (out + gain * x).astype(jnp.bfloat16)
            state_ref[...] = state * rows_of(d_ref[:, span], head_dim)[:, :state_dim] + parts[
                :, i * state_dim:(i + 1) * state_dim]
        return carry

    lax.fori_loop(0, tokens // PAIR, pair, 0)


def local(raw_inputs, state_maps, step_size, log_decay, conv_weight, conv_bias, skip_gain):
    taps = conv_weight.shape[0]
    channels, tokens = raw_inputs.shape
    heads = skip_gain.shape[0]
    head_dim = channels // heads
    state_dim = state_maps.shape[0] // 2
    peers = lax.axis_size("cp")
    tiles = tokens // TILE
    group_rows = GROUP * head_dim
    f32, bf16 = jnp.float32, jnp.bfloat16

    tail = raw_inputs[:, tokens - (taps - 1):].T
    halo = lax.ppermute(tail, "cp", [(s, s + 1) for s in range(peers - 1)])
    vector = jax.ShapeDtypeStruct((heads, tokens), f32)
    e, b, a0, a1, f, d, total, keys, mix = pl.pallas_call(
        functools.partial(prepare_kernel, state_dim),
        out_shape=[vector] * 6 + [
            jax.ShapeDtypeStruct((heads, TILE), f32),
            jax.ShapeDtypeStruct((tiles // 2, PAIR, 2 * state_dim), bf16),
            jax.ShapeDtypeStruct((tiles, TILE + state_dim, 2 * TILE), bf16),
        ],
        cost_estimate=pl.CostEstimate(flops=100000000, bytes_accessed=6000000, transcendentals=0),
    )(log_decay, step_size, state_maps)
    side = jnp.concatenate([0.5 * conv_weight, 0.5 * conv_bias[None], halo.astype(f32)], axis=0)

    grid = heads // GROUP
    wide = lambda cols: pl.BlockSpec((group_rows, cols), lambda g: (g, 0))
    small = pl.BlockSpec((group_rows // 2, 2 * state_dim), lambda g: (g, 0))
    vec = pl.BlockSpec((GROUP, tokens), lambda g: (g, 0))
    vec1 = pl.BlockSpec((GROUP, TILE), lambda g: (g, 0))
    full = lambda array: pl.BlockSpec(array.shape, lambda g: (0,) * array.ndim)
    x, part, message = pl.pallas_call(
        functools.partial(state_kernel, head_dim, state_dim),
        grid=(grid,),
        in_specs=[wide(tokens), pl.BlockSpec((side.shape[0], group_rows), lambda g: (0, g)), vec, vec, full(keys)],
        out_specs=[wide(tokens), wide(tiles * state_dim), small],
        out_shape=[
            jax.ShapeDtypeStruct((channels, tokens), bf16),
            jax.ShapeDtypeStruct((channels, tiles * state_dim), bf16),
            jax.ShapeDtypeStruct((channels // 2, 2 * state_dim), bf16),
        ],
        scratch_shapes=[pltpu.VMEM((group_rows, TILE), f32), pltpu.VMEM((group_rows, tokens), bf16),
                        pltpu.VMEM((GROUP * 8, tokens), f32)],
        compiler_params=pltpu.CompilerParams(dimension_semantics=("arbitrary",)),
    )(raw_inputs, side, e, d, keys)

    own = channels // 2 // peers
    logs = jnp.repeat(total[:, 0], head_dim // 2).reshape(peers, own)
    high = lax.reduce_precision(logs, 8, 7)
    middle = lax.reduce_precision(logs - high, 8, 7)
    log_rows = jnp.stack([high, middle, logs - high - middle], axis=1).astype(bf16)
    filled = -(-(own + 3) // 16) * 16
    log_rows = jnp.pad(log_rows, ((0, 0), (0, filled - own - 3), (0, 2 * state_dim - own)))
    send = jnp.concatenate([message.reshape(peers, own, 2 * state_dim), log_rows], axis=1)
    squares = -(-peers // TILE) * TILE
    returned = pl.pallas_call(
        functools.partial(exchange_kernel, peers, own),
        out_shape=jax.ShapeDtypeStruct((peers, own, 2 * state_dim), bf16),
        in_specs=[pl.BlockSpec(memory_space=pltpu.VMEM)],
        out_specs=pl.BlockSpec(memory_space=pltpu.VMEM),
        scratch_shapes=[
            pltpu.VMEM((peers, filled, 2 * state_dim), bf16),
            pltpu.VMEM((peers, own, 2 * state_dim), bf16),
            pltpu.VMEM((peers, own, 2 * state_dim), bf16),
            pltpu.VMEM((squares, 2 * state_dim), f32),
        ] + [pltpu.SemaphoreType.DMA((peers,))] * 4,
        compiler_params=pltpu.CompilerParams(collective_id=0, has_side_effects=True),
    )(send)
    enter = returned.reshape(channels // 2, 2 * state_dim)
    gain = jnp.broadcast_to(skip_gain[:, None], (heads, TILE))
    return pl.pallas_call(
        functools.partial(output_kernel, head_dim, state_dim),
        grid=(grid,),
        in_specs=[wide(tokens), wide(tiles * state_dim), small, vec, vec, vec, vec, vec, vec1, full(mix)],
        out_specs=wide(tokens),
        out_shape=jax.ShapeDtypeStruct((channels, tokens), bf16),
        scratch_shapes=[pltpu.VMEM((group_rows, state_dim), f32)],
        compiler_params=pltpu.CompilerParams(dimension_semantics=("arbitrary",)),
    )(x, part, enter, b, a0, a1, f, d, gain, mix)


def solution(mesh):
    placed = (P(None, "cp"), P(None, "cp"), P(None, "cp"), P(None, "cp"), P(), P(), P())
    return jax.shard_map(
        local, mesh=mesh, in_specs=placed, out_specs=P(None, "cp"), check_vma=False
    )
```

```python
import functools

import jax
import jax.numpy as jnp
from jax import lax
from jax.experimental import pallas as pl
from jax.experimental.pallas import tpu as pltpu
from jax.sharding import PartitionSpec as P

HALF = 64
TILE = 128
PAIR = 256
GROUP = 8


def prepare_kernel(state_dim, decay_ref, step_ref, maps_ref, e_ref, b_ref, a0_ref, a1_ref, f_ref, d_ref,
                   total_ref, key_ref, mix_ref):
    tiles = decay_ref.shape[1] // TILE
    heads = decay_ref.shape[0]
    row = lax.broadcasted_iota(jnp.int32, (TILE, TILE), 0)
    col = lax.broadcasted_iota(jnp.int32, (TILE, TILE), 1)
    upper = (row <= col).astype(jnp.float32)
    same = (row <= col) & ((row < HALF) == (col < HALF))
    cross = (row < HALF) & (col >= HALF)
    lane = lax.broadcasted_iota(jnp.int32, (heads, TILE), 1)
    low_cols = lax.broadcasted_iota(jnp.int32, (state_dim, TILE), 1) < HALF
    total = jnp.zeros((heads, TILE), jnp.float32)
    for t in range(tiles):
        span = slice(t * TILE, (t + 1) * TILE)
        sums = jnp.dot(decay_ref[:, span], upper, precision=lax.Precision.HIGHEST,
                       preferred_element_type=jnp.float32)
        step = step_ref[:, span]
        first = jnp.broadcast_to(sums[:, HALF // 2 - 1:HALF // 2], (heads, TILE))
        second = jnp.broadcast_to(sums[:, HALF + HALF // 2 - 1:HALF + HALF // 2], (heads, TILE))
        end = jnp.broadcast_to(sums[:, TILE - 1:], (heads, TILE))
        middle = jnp.where(lane < HALF, first, second)
        e_ref[:, span] = jnp.exp(end - sums) * step
        b_ref[:, span] = jnp.exp(middle - sums) * step
        a0_ref[:, span] = jnp.exp(sums - middle)
        a1_ref[:, span] = jnp.where(lane < HALF, 0.0, jnp.exp(jnp.where(lane < HALF, 0.0, sums - first)))
        f_ref[:, span] = jnp.exp(first)
        d_ref[:, span] = jnp.exp(end)
        total = total + end
        keys = maps_ref[:state_dim, span]
        queries = maps_ref[state_dim:, span]
        keys_t = keys.astype(jnp.float32).T.astype(jnp.bfloat16)
        affinity = jnp.dot(keys_t, queries, preferred_element_type=jnp.float32)
        zero_keys = jnp.zeros_like(keys_t)
        side = [keys_t, zero_keys] if t % 2 == 0 else [zero_keys, keys_t]
        key_ref[t // 2, (t % 2) * TILE:(t % 2 + 1) * TILE, :] = jnp.concatenate(side, axis=1)
        mix_ref[t, :TILE, :TILE] = jnp.where(same, affinity, 0.0).astype(jnp.bfloat16)
        mix_ref[t, :TILE, TILE:] = jnp.where(cross, affinity, 0.0).astype(jnp.bfloat16)
        wide = queries.astype(jnp.float32)
        mix_ref[t, TILE:, :TILE] = jnp.where(low_cols, wide, 0.0).astype(jnp.bfloat16)
        mix_ref[t, TILE:, TILE:] = jnp.where(low_cols, 0.0, wide).astype(jnp.bfloat16)
    total_ref[...] = total


def rows_of(vector, head_dim):
    count, width = vector.shape
    return jnp.broadcast_to(vector[:, None, :], (count, head_dim, width)).reshape(count * head_dim, width)


def state_kernel(head_dim, state_dim, raw_ref, side_ref, e_ref, d_ref, key_ref, x_ref, part_ref, message_ref,
                 column_ref, scaled_ref, spread_ref, weight_ref):
    rows, tokens = raw_ref.shape
    tiles = tokens // TILE
    halves = jnp.where(lax.broadcasted_iota(jnp.int32, side_ref.shape, 0) < 5, 0.5, 1.0)
    side = side_ref[...] * halves
    padded = jnp.concatenate([jnp.zeros((TILE - side.shape[0], rows), jnp.float32), side], axis=0)
    column_ref[...] = padded.T
    spread_ref[...] = rows_of(e_ref[...], 8)
    base = TILE - side.shape[0]
    for k in range(5):
        weight_ref[k] = jnp.broadcast_to(column_ref[:, base + k:base + k + 1], (rows, TILE))
    step_rows = head_dim // 2

    def convolve(group, carry):
        start = pl.multiple_of(group * step_rows, step_rows)
        head = group // 2
        lane = lax.broadcasted_iota(jnp.int32, (step_rows, TILE), 1)
        columns = column_ref[pl.ds(start, step_rows), :]
        w0, w1, w2, w3, bias = [weight_ref[k, pl.ds(start, step_rows), :] for k in range(5)]
        before1 = pltpu.roll(columns, 1, 1)
        before2 = pltpu.roll(w1 * columns + w0 * before1, 2, 1)
        for t in range(tiles):
            span = slice(t * TILE, (t + 1) * TILE)
            w0, w1, w2, w3, bias = [weight_ref[k, pl.ds(start, step_rows), :] for k in range(5)]
            now = raw_ref[pl.ds(start, step_rows), span].astype(jnp.float32)
            turned = pltpu.roll(now, 1, 1)
            late1 = jnp.where(lane < 1, before1, turned)
            before1 = turned
            turned = pltpu.roll(w1 * now + w0 * late1, 2, 1)
            late2 = jnp.where(lane < 2, before2, turned)
            before2 = turned
            half = (bias + w3 * now) + (w2 * late1 + late2)
            value = half + half * jnp.tanh(half)
            weight = jnp.concatenate([spread_ref[pl.ds(pl.multiple_of(head * 8, 8), 8), span]] * (step_rows // 8), axis=0)
            x_ref[pl.ds(start, step_rows), span] = value.astype(jnp.bfloat16)
            scaled_ref[pl.ds(start, step_rows), span] = (value * weight).astype(jnp.bfloat16)
        return carry

    lax.fori_loop(0, rows // step_rows, convolve, 0)
    low = lax.broadcasted_iota(jnp.int32, (d_ref.shape[0], TILE), 1) < state_dim
    both = jnp.zeros((rows, TILE), jnp.float32)
    last = d_ref[:, :TILE]
    for k in range(tokens // PAIR):
        part = jnp.dot(scaled_ref[:, k * PAIR:(k + 1) * PAIR], key_ref[k], preferred_element_type=jnp.float32)
        part_ref[:, k * TILE:(k + 1) * TILE] = part.astype(jnp.bfloat16)
        even = d_ref[:, 2 * k * TILE:(2 * k + 1) * TILE]
        odd = d_ref[:, (2 * k + 1) * TILE:(2 * k + 2) * TILE]
        both = part if k == 0 else rows_of(even * jnp.where(low, last, odd), head_dim) * both + part
        last = odd
    state = both[:, :state_dim] * rows_of(last, head_dim)[:, :state_dim] + both[:, state_dim:]
    message_ref[...] = packed(state, head_dim).astype(jnp.bfloat16)


def packed(state, head_dim):
    rows, width = state.shape
    pieces = state.reshape(rows // head_dim, 2, head_dim // 2, width)
    return jnp.concatenate([pieces[:, 0], pieces[:, 1]], axis=2).reshape(rows // 2, 2 * width)


def unpacked(pairs, head_dim):
    rows, width = pairs.shape
    pieces = pairs.reshape(2 * rows // head_dim, head_dim // 2, width)
    return jnp.concatenate([pieces[:, :, :width // 2], pieces[:, :, width // 2:]], axis=1).reshape(
        2 * rows, width // 2)


def exchange_kernel(peers, own, state_ref, extra_ref, out_ref, message_ref, got_ref, reply_ref, back_ref, log_ref,
                    send1, recv1, send2, recv2):
    me = lax.axis_index("cp")
    barrier = pltpu.get_barrier_semaphore()
    message_ref[:, :own] = state_ref[...]
    message_ref[:, own:] = extra_ref[...]

    def greet(k, carry):
        pl.semaphore_signal(barrier, inc=1, device_id=(lax.rem(me + k, peers),),
                            device_id_type=pl.DeviceIdType.MESH)
        return carry

    lax.fori_loop(1, peers, greet, 0)
    pl.semaphore_wait(barrier, peers - 1)

    def outward(k):
        peer = lax.rem(me + k, peers)
        return pltpu.make_async_remote_copy(
            src_ref=message_ref.at[peer], dst_ref=got_ref.at[me], send_sem=send1.at[peer], recv_sem=recv1.at[me],
            device_id=(peer,), device_id_type=pl.DeviceIdType.MESH)

    def inward(k):
        peer = lax.rem(me + k, peers)
        return pltpu.make_async_remote_copy(
            src_ref=message_ref.at[peer], dst_ref=got_ref.at[peer], send_sem=send1.at[peer], recv_sem=recv1.at[peer],
            device_id=(peer,), device_id_type=pl.DeviceIdType.MESH)

    def reply(k):
        peer = lax.rem(me + k, peers)
        return pltpu.make_async_remote_copy(
            src_ref=reply_ref.at[peer], dst_ref=back_ref.at[me], send_sem=send2.at[peer], recv_sem=recv2.at[me],
            device_id=(peer,), device_id_type=pl.DeviceIdType.MESH)

    def answer(k):
        peer = lax.rem(me + k, peers)
        return pltpu.make_async_remote_copy(
            src_ref=reply_ref.at[peer], dst_ref=back_ref.at[peer], send_sem=send2.at[peer], recv_sem=recv2.at[peer],
            device_id=(peer,), device_id_type=pl.DeviceIdType.MESH)

    def each(action):
        def step(k, carry):
            action(k)
            return carry
        lax.fori_loop(1, peers, step, 0)

    each(lambda k: outward(k).start())
    got_ref[me] = message_ref[me]
    each(lambda k: inward(k).wait_recv())
    log_ref[...] = jnp.zeros_like(log_ref)
    for d in range(peers):
        logs = got_ref[d, own:own + 3].astype(jnp.float32)
        log_ref[d:d + 1] = (logs[0:1] + logs[1:2]) + logs[2:3]
    decays = jnp.exp(log_ref[...]).T
    running = jnp.zeros((own, got_ref.shape[2]), jnp.float32)
    for d in range(peers):
        reply_ref[d] = running.astype(jnp.bfloat16)
        running = decays[:own, d:d + 1] * running + got_ref[d, :own].astype(jnp.float32)
    each(lambda k: reply(k).start())
    back_ref[me] = reply_ref[me]
    each(lambda k: answer(k).wait_recv())
    out_ref[...] = back_ref[...]
    each(lambda k: outward(k).wait_send())
    each(lambda k: reply(k).wait_send())


def output_kernel(head_dim, state_dim, x_ref, part_ref, enter_ref, b_ref, a0_ref, a1_ref, f_ref, d_ref, gain_ref,
                  mix_ref, out_ref, state_ref):
    tokens = x_ref.shape[1]
    state_ref[...] = unpacked(enter_ref[...].astype(jnp.float32), head_dim)
    gain = rows_of(gain_ref[...], head_dim)

    def pair(k, carry):
        parts = part_ref[:, pl.ds(pl.multiple_of(k * TILE, TILE), TILE)].astype(jnp.float32)
        for i in range(2):
            span = pl.ds(pl.multiple_of(k * PAIR + i * TILE, TILE), TILE)
            x = x_ref[:, span].astype(jnp.float32)
            scaled = (x * rows_of(b_ref[:, span], head_dim)).astype(jnp.bfloat16)
            state = state_ref[...]
            entering = (state * rows_of(f_ref[:, span], head_dim)[:, :state_dim]).astype(jnp.bfloat16)
            left = jnp.concatenate([scaled, entering], axis=1)
            mixed = jnp.dot(left, mix_ref[2 * k + i], preferred_element_type=jnp.float32)
            out = mixed[:, :TILE] * rows_of(a0_ref[:, span], head_dim)
            out = out + mixed[:, TILE:] * rows_of(a1_ref[:, span], head_dim)
            out_ref[:, span] = (out + gain * x).astype(jnp.bfloat16)
            state_ref[...] = state * rows_of(d_ref[:, span], head_dim)[:, :state_dim] + parts[
                :, i * state_dim:(i + 1) * state_dim]
        return carry

    lax.fori_loop(0, tokens // PAIR, pair, 0)


def local(raw_inputs, state_maps, step_size, log_decay, conv_weight, conv_bias, skip_gain):
    taps = conv_weight.shape[0]
    channels, tokens = raw_inputs.shape
    heads = skip_gain.shape[0]
    head_dim = channels // heads
    state_dim = state_maps.shape[0] // 2
    peers = lax.axis_size("cp")
    tiles = tokens // TILE
    group_rows = GROUP * head_dim
    f32, bf16 = jnp.float32, jnp.bfloat16

    tail = raw_inputs[:, tokens - (taps - 1):].T
    halo = lax.ppermute(tail, "cp", [(s, s + 1) for s in range(peers - 1)])
    vector = jax.ShapeDtypeStruct((heads, tokens), f32)
    e, b, a0, a1, f, d, total, keys, mix = pl.pallas_call(
        functools.partial(prepare_kernel, state_dim),
        out_shape=[vector] * 6 + [
            jax.ShapeDtypeStruct((heads, TILE), f32),
            jax.ShapeDtypeStruct((tiles // 2, PAIR, 2 * state_dim), bf16),
            jax.ShapeDtypeStruct((tiles, TILE + state_dim, 2 * TILE), bf16),
        ],
        cost_estimate=pl.CostEstimate(flops=100000000, bytes_accessed=6000000, transcendentals=0),
    )(log_decay, step_size, state_maps)
    side = jnp.concatenate([conv_weight, conv_bias[None], halo.astype(f32)], axis=0)

    grid = heads // GROUP
    wide = lambda cols: pl.BlockSpec((group_rows, cols), lambda g: (g, 0))
    small = pl.BlockSpec((group_rows // 2, 2 * state_dim), lambda g: (g, 0))
    vec = pl.BlockSpec((GROUP, tokens), lambda g: (g, 0))
    vec1 = pl.BlockSpec((GROUP, TILE), lambda g: (g, 0))
    full = lambda array: pl.BlockSpec(array.shape, lambda g: (0,) * array.ndim)
    x, part, message = pl.pallas_call(
        functools.partial(state_kernel, head_dim, state_dim),
        grid=(grid,),
        in_specs=[wide(tokens), pl.BlockSpec((side.shape[0], group_rows), lambda g: (0, g)), vec, vec, full(keys)],
        out_specs=[wide(tokens), wide(tiles * state_dim), small],
        out_shape=[
            jax.ShapeDtypeStruct((channels, tokens), bf16),
            jax.ShapeDtypeStruct((channels, tiles * state_dim), bf16),
            jax.ShapeDtypeStruct((channels // 2, 2 * state_dim), bf16),
        ],
        scratch_shapes=[pltpu.VMEM((group_rows, TILE), f32), pltpu.VMEM((group_rows, tokens), bf16),
                        pltpu.VMEM((GROUP * 8, tokens), f32),
                        pltpu.VMEM((5, group_rows, TILE), f32)],
        compiler_params=pltpu.CompilerParams(dimension_semantics=("arbitrary",)),
    )(raw_inputs, side, e, d, keys)

    own = channels // 2 // peers
    logs = jnp.repeat(total[:, 0], head_dim // 2).reshape(peers, own)
    high = lax.reduce_precision(logs, 8, 7)
    middle = lax.reduce_precision(logs - high, 8, 7)
    log_rows = jnp.stack([high, middle, logs - high - middle], axis=1).astype(bf16)
    filled = -(-(own + 3) // 16) * 16
    log_rows = jnp.pad(log_rows, ((0, 0), (0, filled - own - 3), (0, 2 * state_dim - own)))
    squares = -(-peers // TILE) * TILE
    returned = pl.pallas_call(
        functools.partial(exchange_kernel, peers, own),
        out_shape=jax.ShapeDtypeStruct((peers, own, 2 * state_dim), bf16),
        in_specs=[pl.BlockSpec(memory_space=pltpu.VMEM)] * 2,
        out_specs=pl.BlockSpec(memory_space=pltpu.VMEM),
        scratch_shapes=[
            pltpu.VMEM((peers, filled, 2 * state_dim), bf16),
            pltpu.VMEM((peers, filled, 2 * state_dim), bf16),
            pltpu.VMEM((peers, own, 2 * state_dim), bf16),
            pltpu.VMEM((peers, own, 2 * state_dim), bf16),
            pltpu.VMEM((squares, 2 * state_dim), f32),
        ] + [pltpu.SemaphoreType.DMA((peers,))] * 4,
        compiler_params=pltpu.CompilerParams(collective_id=0, has_side_effects=True),
    )(message.reshape(peers, own, 2 * state_dim), log_rows)
    enter = returned.reshape(channels // 2, 2 * state_dim)
    gain = jnp.broadcast_to(skip_gain[:, None], (heads, TILE))
    return pl.pallas_call(
        functools.partial(output_kernel, head_dim, state_dim),
        grid=(grid,),
        in_specs=[wide(tokens), wide(tiles * state_dim), small, vec, vec, vec, vec, vec, vec1, full(mix)],
        out_specs=wide(tokens),
        out_shape=jax.ShapeDtypeStruct((channels, tokens), bf16),
        scratch_shapes=[pltpu.VMEM((group_rows, state_dim), f32)],
        compiler_params=pltpu.CompilerParams(dimension_semantics=("arbitrary",)),
    )(x, part, enter, b, a0, a1, f, d, gain, mix)


def solution(mesh):
    placed = (P(None, "cp"), P(None, "cp"), P(None, "cp"), P(None, "cp"), P(), P(), P())
    return jax.shard_map(
        local, mesh=mesh, in_specs=placed, out_specs=P(None, "cp"), check_vma=False
    )
```
